32 devices in a mesh: gx: 2 (over y), gy: 4 (over x, core), gz: 4 (over z).
Axes of the slice: x: 2, y: 2, z: 4, core: 2. Of those that a mesh axis runs over, the one named last changes fastest.
Arguments:
- tokens: bfloat16 [256, 8192], P('gx', 'gy'), may hold values from -6 to 6
- cotangent: bfloat16 [256, 8192], P('gx', 'gy'), may hold values from -6 to 6
- gate_weight: bfloat16 [8192, 28672], P('gy', ('gx', 'gz')), may hold values from -5.7452426 to 5.7452426
- up_weight: bfloat16 [8192, 28672], P('gy', ('gx', 'gz')), may hold values from -5.7452426 to 5.7452426
- down_weight: bfloat16 [28672, 8192], P(('gx', 'gz'), 'gy'), may hold values from -3.0709613 to 3.0709613
- gate_reduce: bfloat16 [8192, 32], P('gy'), may hold values from -0.0625 to 0.0625
- gate_expand: bfloat16 [32, 28672], P(None, ('gx', 'gz')), may hold values from -5 to 5
- gate_magnitude: float32 [28672], P(('gx', 'gz')), may hold values from 0.5 to 2
- up_reduce: bfloat16 [8192, 32], P('gy'), may hold values from -0.0625 to 0.0625
- up_expand: bfloat16 [32, 28672], P(None, ('gx', 'gz')), may hold values from -5 to 5
- up_magnitude: float32 [28672], P(('gx', 'gz')), may hold values from 0.5 to 2
- down_reduce: bfloat16 [28672, 32], P(('gx', 'gz')), may hold values from -0.03125 to 0.03125
- down_expand: bfloat16 [32, 8192], P(None, 'gy'), may hold values from -5 to 5
- down_magnitude: float32 [8192], P('gy'), may hold values from 0.5 to 2
Outputs:
- output: bfloat16 [256, 8192], P('gx', 'gy')
- grad_tokens: bfloat16 [256, 8192], P('gx', 'gy')
- grad_gate_reduce: float32 [8192, 32], P('gy')
- grad_gate_expand: float32 [32, 28672], P(None, ('gx', 'gz'))
- grad_gate_magnitude: float32 [28672], P(('gx', 'gz'))
- grad_up_reduce: float32 [8192, 32], P('gy')
- grad_up_expand: float32 [32, 28672], P(None, ('gx', 'gz'))
- grad_up_magnitude: float32 [28672], P(('gx', 'gz'))
- grad_down_reduce: float32 [28672, 32], P(('gx', 'gz'))
- grad_down_expand: float32 [32, 8192], P(None, 'gy')
- grad_down_magnitude: float32 [8192], P('gy')
The draws below stay inside these ranges and needn't reach their ends.
All inputs are finite; a program needn't handle non-finite values.
Results may differ from the reference program's by a relative error of at most 0.012.
Values may be sent and summed in bfloat16 or wider, within the bound.
A program may use at most 128 MiB of HBM per device.

```python
import math
import jax
import jax.numpy as jnp
from jax import lax

D = 8192
FF = 28672
R = 32
TOKENS = 256


def weight_law(key, in_rows, columns):
    key_base = jax.random.fold_in(key, 0)
    key_row = jax.random.fold_in(key, 2)
    key_col = jax.random.fold_in(key, 3)
    position = jnp.arange(in_rows, dtype=jnp.float32) / in_rows
    spread = 1.15
    entries = jax.random.truncated_normal(key_base, -4.0, 4.0, (in_rows, columns), jnp.float32)
    row_scale = jnp.exp(math.log(3.0) * position + jax.random.uniform(key_row, (in_rows,), jnp.float32, -spread, spread))
    col_scale = jnp.exp(jax.random.uniform(key_col, (columns,), jnp.float32, 0.0, math.log(10.0)))
    values = entries * row_scale[:, None] * col_scale[None, :] / math.sqrt(in_rows)
    return values.astype(jnp.bfloat16)


def draw_gate_weight(key, part):
    return weight_law(jax.random.fold_in(key, 11), D, FF)


def draw_up_weight(key, part):
    return weight_law(jax.random.fold_in(key, 12), D, FF)


def draw_down_weight(key, part):
    return weight_law(jax.random.fold_in(key, 13), FF, D)


def shard_levels(rng, shape, cuts, least, largest):
    factor_of, own = 1.0, jax.random.fold_in(rng, 6)
    for dim, blocks in cuts:
        heights = jnp.exp(jax.random.uniform(jax.random.fold_in(own, dim), (blocks,), jnp.float32, least / len(cuts), largest / len(cuts)))
        factor_of = factor_of * jnp.repeat(heights, shape[dim] // blocks).reshape([-1 if axis == dim else 1 for axis in range(len(shape))])
    return factor_of


def scatter_about(key, dims, width, bound, shards=(), held_as=jnp.bfloat16):
    result = width * jax.random.normal(key, dims, jnp.float32)
    if shards:
        result = result * shard_levels(key, dims, shards, -0.22, 0.18)
    return jnp.clip(result, -bound, bound).astype(held_as)


def setup_inputs(seed: int = 0) -> dict:
    streams_of = jax.random.split(jax.random.key(seed), 15)
    return {
        "tokens": scatter_about(streams_of[0], (TOKENS, D), 1.0, 6.0, ((0, 2), (1, 4))),
        "cotangent": scatter_about(streams_of[1], (TOKENS, D), 1.0, 6.0, ((0, 2), (1, 4))),
        "gate_weight": draw_gate_weight(jax.random.fold_in(streams_of[14], 71), 0),
        "up_weight": draw_up_weight(jax.random.fold_in(streams_of[14], 71), 0),
        "down_weight": draw_down_weight(jax.random.fold_in(streams_of[14], 71), 0),
        "gate_reduce": scatter_about(streams_of[5], (D, R), D ** -0.5, 0.0625, ((0, 4),)),
        "gate_expand": scatter_about(streams_of[6], (R, FF), 0.35, 5.0, ((1, 8),)),
        "gate_magnitude": jnp.clip(jnp.exp(math.log(2.0) - 1.3862944 * jax.random.uniform(streams_of[7], (FF,), jnp.float32) ** shard_levels(streams_of[7], (FF,), ((0, 8),), -0.2, 0.2)), 0.5, 2.0),
        "up_reduce": scatter_about(streams_of[8], (D, R), D ** -0.5, 0.0625, ((0, 4),)),
        "up_expand": scatter_about(streams_of[9], (R, FF), 0.35, 5.0, ((1, 8),)),
        "up_magnitude": jnp.clip(jnp.exp(math.log(2.0) - 1.3862944 * jax.random.uniform(streams_of[10], (FF,), jnp.float32) ** shard_levels(streams_of[10], (FF,), ((0, 8),), -0.2, 0.2)), 0.5, 2.0),
        "down_reduce": scatter_about(streams_of[11], (FF, R), FF ** -0.5, 0.03125, ((0, 8),)),
        "down_expand": scatter_about(streams_of[12], (R, D), 0.35, 5.0, ((1, 4),)),
        "down_magnitude": jnp.clip(jnp.exp(math.log(2.0) - 1.3862944 * jax.random.uniform(streams_of[13], (D,), jnp.float32) ** shard_levels(streams_of[13], (D,), ((0, 4),), -0.2, 0.2)), 0.5, 2.0),
    }


EPSILON = 1e-06

def column_norm(weight, reduce_in, expand_out):
    in_rows = weight.shape[0]
    blocks = 16
    weight_blocks = weight.reshape(blocks, in_rows // blocks, weight.shape[1])
    reduce_blocks = reduce_in.reshape(blocks, in_rows // blocks, reduce_in.shape[1])

    def add_block(running, pieces):
        weight_part, reduce_part = pieces
        merged = weight_part.astype(jnp.float32) + jnp.dot(reduce_part, expand_out, preferred_element_type=jnp.float32)
        return (running + lax.optimization_barrier(jnp.sum(merged * merged, axis=0)), None)
    initial = jnp.zeros((weight.shape[1],), jnp.float32)
    running, unused = lax.scan(add_block, initial, (weight_blocks, reduce_blocks))
    return jnp.sqrt(running + EPSILON)

def lowrank_linear(inputs, weight, reduce_in, expand_out):
    low_part = jnp.dot(inputs, reduce_in, preferred_element_type=jnp.float32).astype(jnp.bfloat16)
    linear = jnp.dot(inputs, weight, preferred_element_type=jnp.float32) + jnp.dot(low_part, expand_out, preferred_element_type=jnp.float32)
    return (linear, low_part)

def reference(tokens, cotangent, gate_weight, up_weight, down_weight, gate_reduce, gate_expand, gate_magnitude, up_reduce, up_expand, up_magnitude, down_reduce, down_expand, down_magnitude):
    norm_gate = column_norm(gate_weight, gate_reduce, gate_expand)
    norm_up = column_norm(up_weight, up_reduce, up_expand)
    norm_down = column_norm(down_weight, down_reduce, down_expand)
    scale_gate = gate_magnitude / norm_gate
    scale_up = up_magnitude / norm_up
    scale_down = down_magnitude / norm_down
    gate_lin, gate_low = lowrank_linear(tokens, gate_weight, gate_reduce, gate_expand)
    up_lin, up_low = lowrank_linear(tokens, up_weight, up_reduce, up_expand)
    gate_pre = gate_lin * scale_gate[None, :]
    up_pre = up_lin * scale_up[None, :]
    sigmoid_gate = jax.nn.sigmoid(gate_pre)
    active = gate_pre * sigmoid_gate
    hidden = (active * up_pre).astype(jnp.bfloat16)
    down_lin, down_low = lowrank_linear(hidden, down_weight, down_reduce, down_expand)
    output = (down_lin * scale_down[None, :]).astype(jnp.bfloat16)
    cot_float = cotangent.astype(jnp.float32)
    down_delta = (cot_float * scale_down[None, :]).astype(jnp.bfloat16)
    grad_down_magnitude = lax.optimization_barrier(jnp.sum(cot_float * down_lin, axis=0)) / norm_down
    grad_down_expand = jnp.dot(down_low.T, down_delta, preferred_element_type=jnp.float32)
    down_back = jnp.dot(down_delta, down_expand.T, preferred_element_type=jnp.float32).astype(jnp.bfloat16)
    grad_down_reduce = jnp.dot(hidden.T, down_back, preferred_element_type=jnp.float32)
    hidden_grad = (jnp.dot(down_delta, down_weight.T, preferred_element_type=jnp.float32) + jnp.dot(down_back, down_reduce.T, preferred_element_type=jnp.float32)).astype(jnp.bfloat16)
    hgrad_float = hidden_grad.astype(jnp.float32)
    gate_grad = hgrad_float * up_pre * sigmoid_gate * (1.0 + gate_pre * (1.0 - sigmoid_gate))
    up_grad = hgrad_float * active
    gate_delta = (gate_grad * scale_gate[None, :]).astype(jnp.bfloat16)
    up_delta = (up_grad * scale_up[None, :]).astype(jnp.bfloat16)
    grad_gate_magnitude = lax.optimization_barrier(jnp.sum(gate_grad * gate_lin, axis=0)) / norm_gate
    grad_up_magnitude = lax.optimization_barrier(jnp.sum(up_grad * up_lin, axis=0)) / norm_up
    grad_gate_expand = jnp.dot(gate_low.T, gate_delta, preferred_element_type=jnp.float32)
    grad_up_expand = jnp.dot(up_low.T, up_delta, preferred_element_type=jnp.float32)
    gate_back = jnp.dot(gate_delta, gate_expand.T, preferred_element_type=jnp.float32).astype(jnp.bfloat16)
    up_back = jnp.dot(up_delta, up_expand.T, preferred_element_type=jnp.float32).astype(jnp.bfloat16)
    grad_gate_reduce = jnp.dot(tokens.T, gate_back, preferred_element_type=jnp.float32)
    grad_up_reduce = jnp.dot(tokens.T, up_back, preferred_element_type=jnp.float32)
    grad_tokens = (jnp.dot(gate_delta, gate_weight.T, preferred_element_type=jnp.float32) + jnp.dot(up_delta, up_weight.T, preferred_element_type=jnp.float32) + jnp.dot(gate_back, gate_reduce.T, preferred_element_type=jnp.float32) + jnp.dot(up_back, up_reduce.T, preferred_element_type=jnp.float32)).astype(jnp.bfloat16)
    return (output, grad_tokens, grad_gate_reduce, grad_gate_expand, grad_gate_magnitude, grad_up_reduce, grad_up_expand, grad_up_magnitude, grad_down_reduce, grad_down_expand, grad_down_magnitude)
```

```python
import functools

import jax
import jax.numpy as jnp
from jax import lax
from jax.experimental import pallas as pl
from jax.experimental.pallas import tpu as pltpu
from jax.sharding import PartitionSpec as P

EPSILON = 1e-06
BF16 = jnp.bfloat16
F32 = jnp.float32


def tile_square(weight, reduce_in, expand_out):
    merged = weight.astype(jnp.float32) + jnp.dot(
        reduce_in, expand_out, preferred_element_type=jnp.float32
    )
    return jnp.sum(merged * merged, axis=0)


def share_rows(values, count):
    return lax.dynamic_slice_in_dim(values, lax.axis_index("gz") * count, count, 0)


def contract_last(left, right):
    return lax.dot_general(
        left, right, (((1,), (1,)), ((), ())), preferred_element_type=jnp.float32
    )


def contract_first(left, right):
    return lax.dot_general(
        left, right, (((0,), (0,)), ((), ())), preferred_element_type=jnp.float32
    )


def scatter_pair(part, low_part, axes):
    width = part.shape[1]
    joined = jnp.concatenate(
        [part.astype(jnp.bfloat16), low_part.astype(jnp.bfloat16)], axis=1
    )
    summed = lax.psum_scatter(joined, axes, scatter_dimension=0, tiled=True)
    return summed[:, :width].astype(jnp.float32), summed[:, width:]


def on_device(
    tokens,
    cotangent,
    gate_weight,
    up_weight,
    down_weight,
    gate_reduce,
    gate_expand,
    gate_magnitude,
    up_reduce,
    up_expand,
    up_magnitude,
    down_reduce,
    down_expand,
    down_magnitude,
):
    share_count = tokens.shape[0] // lax.axis_size("gz")
    square_gate = tile_square(gate_weight, gate_reduce, gate_expand)
    square_up = tile_square(up_weight, up_reduce, up_expand)
    square_down = tile_square(down_weight, down_reduce, down_expand)
    norm_down = jnp.sqrt(lax.psum(square_down, ("gx", "gz")) + EPSILON)
    scale_down = down_magnitude / norm_down
    all_tokens = lax.all_gather(tokens, "gx", axis=0, tiled=True)
    part_gate = jnp.dot(all_tokens, gate_weight, preferred_element_type=jnp.float32)
    part_up = jnp.dot(all_tokens, up_weight, preferred_element_type=jnp.float32)
    low_gate_part = jnp.dot(all_tokens, gate_reduce, preferred_element_type=jnp.float32)
    low_up_part = jnp.dot(all_tokens, up_reduce, preferred_element_type=jnp.float32)
    gate_lin, gate_low = scatter_pair(part_gate, low_gate_part, "gy")
    up_lin, up_low = scatter_pair(part_up, low_up_part, "gy")
    summed_gate, summed_up = lax.psum((square_gate, square_up), "gy")
    norm_gate = jnp.sqrt(summed_gate + EPSILON)
    norm_up = jnp.sqrt(summed_up + EPSILON)
    scale_gate = gate_magnitude / norm_gate
    scale_up = up_magnitude / norm_up
    gate_lin = gate_lin + jnp.dot(gate_low, gate_expand, preferred_element_type=jnp.float32)
    up_lin = up_lin + jnp.dot(up_low, up_expand, preferred_element_type=jnp.float32)
    gate_pre = gate_lin * scale_gate[None, :]
    up_pre = up_lin * scale_up[None, :]
    sigmoid_gate = jax.nn.sigmoid(gate_pre)
    active = gate_pre * sigmoid_gate
    hidden = (active * up_pre).astype(jnp.bfloat16)
    all_hidden = lax.all_gather(hidden, "gy", axis=0, tiled=True)
    part_down = jnp.dot(all_hidden, down_weight, preferred_element_type=jnp.float32)
    low_down_part = jnp.dot(all_hidden, down_reduce, preferred_element_type=jnp.float32)
    down_lin, down_low = scatter_pair(part_down, low_down_part, ("gx", "gz"))
    down_lin = down_lin + jnp.dot(down_low, down_expand, preferred_element_type=jnp.float32)
    output = lax.all_gather(
        (down_lin * scale_down[None, :]).astype(jnp.bfloat16), "gz", axis=0, tiled=True
    )
    cot_float = cotangent.astype(jnp.float32)
    down_delta = (cot_float * scale_down[None, :]).astype(jnp.bfloat16)
    cot_share = share_rows(cot_float, share_count)
    delta_share = share_rows(down_delta, share_count)
    grad_down_magnitude = jnp.sum(cot_share * down_lin, axis=0) / norm_down
    grad_down_expand = contract_first(down_low, delta_share)
    grad_down_magnitude, grad_down_expand = lax.psum(
        (grad_down_magnitude, grad_down_expand), ("gx", "gz")
    )
    all_delta = lax.all_gather(down_delta, "gx", axis=0, tiled=True)
    part_hidden_grad = contract_last(all_delta, down_weight)
    part_down_back = contract_last(all_delta, down_expand)
    hidden_gradsum, down_back = scatter_pair(part_hidden_grad, part_down_back, "gy")
    hidden_grad = (hidden_gradsum + contract_last(down_back, down_reduce)).astype(jnp.bfloat16)
    hgrad_float = hidden_grad.astype(jnp.float32)
    gate_grad = hgrad_float * up_pre * sigmoid_gate * (1.0 + gate_pre * (1.0 - sigmoid_gate))
    up_grad = hgrad_float * active
    gate_delta = (gate_grad * scale_gate[None, :]).astype(jnp.bfloat16)
    up_delta = (up_grad * scale_up[None, :]).astype(jnp.bfloat16)
    grad_gate_magnitude = jnp.sum(gate_grad * gate_lin, axis=0) / norm_gate
    grad_up_magnitude = jnp.sum(up_grad * up_lin, axis=0) / norm_up
    grad_gate_magnitude, grad_up_magnitude = lax.psum(
        (grad_gate_magnitude, grad_up_magnitude), "gy"
    )
    rank = gate_low.shape[1]
    all_low = lax.all_gather(
        jnp.concatenate([gate_low, up_low, down_back], axis=1), "gy", axis=0, tiled=True
    )
    all_gate_delta, all_up_delta = (
        lax.all_gather(gate_delta, "gy", axis=0, tiled=True),
        lax.all_gather(up_delta, "gy", axis=0, tiled=True),
    )
    grad_gate_expand = contract_first(all_low[:, :rank], all_gate_delta)
    grad_up_expand = contract_first(all_low[:, rank : 2 * rank], all_up_delta)
    grad_down_reduce = contract_first(all_hidden, all_low[:, 2 * rank :])
    part_input = contract_last(all_gate_delta, gate_weight) + contract_last(all_up_delta, up_weight)
    part_gate_back = contract_last(all_gate_delta, gate_expand)
    part_up_back = contract_last(all_up_delta, up_expand)
    input_sum, back_pair = scatter_pair(
        part_input, jnp.concatenate([part_gate_back, part_up_back], axis=1), ("gx", "gz")
    )
    gate_back = back_pair[:, :rank]
    up_back = back_pair[:, rank:]
    grad_tokens = lax.all_gather(
        (
            input_sum + contract_last(gate_back, gate_reduce) + contract_last(up_back, up_reduce)
        ).astype(jnp.bfloat16),
        "gz",
        axis=0,
        tiled=True,
    )
    token_share = share_rows(tokens, share_count)
    grad_gate_reduce = contract_first(token_share, gate_back)
    grad_up_reduce = contract_first(token_share, up_back)
    grad_gate_reduce, grad_up_reduce = lax.psum((grad_gate_reduce, grad_up_reduce), ("gx", "gz"))
    return (
        output,
        grad_tokens,
        grad_gate_reduce,
        grad_gate_expand,
        grad_gate_magnitude,
        grad_up_reduce,
        grad_up_expand,
        grad_up_magnitude,
        grad_down_reduce,
        grad_down_expand,
        grad_down_magnitude,
    )


LANES = 128


def dot(left, right):
    return jnp.dot(left, right, preferred_element_type=F32)


def kernel(
    tok_hbm, cot_hbm, wg_hbm, wu_hbm, wd_hbm, ag_hbm, au_hbm, bd_hbm, bg_hbm, bu_hbm, ad_hbm,
    mg_hbm, mu_hbm, md_hbm,
    out_hbm, gtok_hbm, grg_hbm, gru_hbm, gde_hbm, geg_hbm, geu_hbm, gdr_hbm,
    gmg_hbm, gmu_hbm, gdm_hbm,
    wide, deep, m_gu, m_d, gm_out, gd_out,
    wg, wu, wd, xt, dl, part, xr, hid, cs, acc, ysend, ykeep, yrecv, z1r, z2r,
    obuf, cot_mine, low, la, lar, back, lb, lbr, nds, ngs, scale_gu, gms, gmr, gds, extra,
    w_sem, in_sem, in_send, in_recv, cs_sem, c_recv, x_send, x_recv, ag_send, ag_recv,
    yz_send, yz_recv, nd_send, gd_send, nd_recv, ng_send, ng_recv, la_send, la_recv,
    lb_send, lb_recv, gm_sem, out_sem, credit,
):
    gx, gy, gz = lax.axis_index("gx"), lax.axis_index("gy"), lax.axis_index("gz")
    core = lax.rem(gy, 2)
    bit0, bit1 = lax.rem(gz, 2), gz // 2
    core_peer = {"gy": gy + 1 - 2 * core}
    x_peer = {"gy": lax.rem(gy + 2, 4)}
    y_peer = {"gx": 1 - gx}
    z1_peer = {"gz": gz + 1 - 2 * bit0}
    z2_peer = {"gz": lax.rem(gz + 2, 4)}
    half_t, width = xt.shape[1], xt.shape[2]
    quarter = half_t // 2
    hidden_l = wg.shape[1]
    rank = gde_hbm.shape[0]
    fc = cs.shape[2]
    nc = hidden_l // fc
    dt = 512 if width % 512 == 0 else width
    nt = width // dt
    mine = pl.ds(pl.multiple_of(core * quarter, quarter), quarter)

    def cols(c):
        return pl.ds(pl.multiple_of(c * fc, fc), fc)

    def tile(t):
        return pl.ds(pl.multiple_of(t * dt, dt), dt)

    def remote(src, dst, send, recv, peer):
        return pltpu.make_async_remote_copy(
            src_ref=src, dst_ref=dst, send_sem=send, recv_sem=recv,
            device_id=peer, device_id_type=pl.DeviceIdType.MESH,
        )

    def group_peer(i):
        place = lax.rem(gx * 4 + gz + i, 8)
        return {"gx": place // 4, "gz": lax.rem(place, 4)}, place

    barrier = pltpu.get_barrier_semaphore()
    for i in range(1, 4):
        pl.semaphore_signal(barrier, inc=1, device_id={"gy": lax.rem(gy + i, 4)}, device_id_type=pl.DeviceIdType.MESH)
    for i in range(1, 8):
        pl.semaphore_signal(barrier, inc=1, device_id=group_peer(i)[0], device_id_type=pl.DeviceIdType.MESH)

    own_tok = pltpu.make_async_copy(tok_hbm, xt.at[gx], in_sem.at[0])
    own_cot = pltpu.make_async_copy(cot_hbm, dl.at[gx], in_sem.at[1])
    block = (bit0 * 2 + bit1) * (half_t // 4)
    my_rows = pl.ds(pl.multiple_of(block, half_t // 4), half_t // 4)
    cot_rows = pltpu.make_async_copy(cot_hbm.at[my_rows], cot_mine, in_sem.at[2])
    own_tok.start()
    factors = [
        pltpu.make_async_copy(src, buf.at[n * rank : (n + 1) * rank], in_sem.at[3 + i])
        for i, (src, buf, n) in enumerate((
            (ag_hbm, wide, 0), (au_hbm, wide, 1), (bg_hbm, deep, 0), (bu_hbm, deep, 1),
            (bd_hbm, wide, 2), (ad_hbm, deep, 2),
        ))
    ]
    factors += [
        pltpu.make_async_copy(src, dst, in_sem.at[9 + i])
        for i, (src, dst) in enumerate(((mg_hbm, m_gu.at[0]), (mu_hbm, m_gu.at[1]), (md_hbm, m_d)))
    ]
    for copy in factors[:4]:
        copy.start()

    def load_w(k, c):
        if k == 0:
            return pltpu.make_async_copy(wg_hbm.at[:, cols(c)], wg.at[:, cols(c)], w_sem.at[0, c])
        if k == 1:
            return pltpu.make_async_copy(wu_hbm.at[:, cols(c)], wu.at[:, cols(c)], w_sem.at[1, c])
        return pltpu.make_async_copy(wd_hbm.at[cols(c)], wd.at[cols(c)], w_sem.at[2, c])

    for c in range(2):
        load_w(0, c).start()
        load_w(1, c).start()
    for copy in factors[4:]:
        copy.start()
    wide[3 * rank :] = jnp.zeros((wide.shape[0] - 3 * rank, width), BF16)
    deep[3 * rank :] = jnp.zeros((deep.shape[0] - 3 * rank, hidden_l), BF16)
    pl.semaphore_wait(barrier, 10)
    send_tok = remote(tok_hbm, xt.at[gx], in_send.at[0], in_recv.at[0], y_peer)
    send_cot = remote(cot_hbm, dl.at[gx], in_send.at[1], in_recv.at[1], y_peer)
    send_tok.start()
    send_cot.start()
    own_cot.start()
    cot_rows.start()

    lane = lax.broadcasted_iota(jnp.int32, (half_t, low.shape[2]), 1)
    is_gate = lane < rank

    def low_of(h):
        low[h] = jnp.where(lane < 2 * rank, contract_last(xt[h], wide[...]), 0.0)

    def unit_id(k, h, c):
        return (k * 2 + h) * nc + c

    def core_copy(k, h, c, slot):
        return remote(
            cs.at[slot], part.at[k, h, mine, cols(c)], cs_sem.at[slot],
            c_recv.at[unit_id(k, h, c)], core_peer,
        )

    other_rows = pl.ds(pl.multiple_of((1 - core) * quarter, quarter), quarter)

    def x_copy(k, h, c):
        return remote(
            part.at[k, h, mine, cols(c)], xr.at[k, h, :, cols(c)],
            x_send.at[unit_id(k, h, c)], x_recv.at[unit_id(k, h, c)], x_peer,
        )

    def emit_unit(k, h, c, slot, value, reuse):
        lo, hi = value[:quarter], value[quarter:]
        part[k, h, mine, cols(c)] = jnp.where(core == 0, lo, hi).astype(BF16)

        @pl.when(reuse)
        def _():
            core_copy(k, h, c, slot).wait_send()

        cs[slot] = jnp.where(core == 0, hi, lo).astype(BF16)
        core_copy(k, h, c, slot).start()

    def finish_unit(k, h, c):
        pltpu.make_async_remote_copy(
            src_ref=cs.at[0], dst_ref=part.at[k, h, other_rows, cols(c)], send_sem=cs_sem.at[0],
            recv_sem=c_recv.at[unit_id(k, h, c)], device_id=core_peer,
            device_id_type=pl.DeviceIdType.MESH,
        ).wait_recv()
        total = part[k, h, mine, cols(c)].astype(F32) + part[k, h, other_rows, cols(c)].astype(F32)
        part[k, h, mine, cols(c)] = total.astype(BF16)
        x_copy(k, h, c).start()

    def gate_up(h, first):
        x_low = low[h]
        low_gate = jnp.where(is_gate, x_low, 0.0).astype(BF16)
        low_up = jnp.where(is_gate, 0.0, x_low).astype(BF16)

        def body(c, _):
            if first:
                load_w(0, c).wait()
                load_w(1, c).wait()

                @pl.when(c + 2 < nc)
                def _():
                    load_w(0, c + 2).start()
                    load_w(1, c + 2).start()

                @pl.when(c + 2 >= nc)
                def _():
                    load_w(2, c + 2 - nc).start()

            for k, w, lw in ((0, wg, low_gate), (1, wu, low_up)):
                value = dot(xt[h], w[:, cols(c)]) + dot(lw, deep[:, cols(c)])
                slot = lax.rem(c, 2) * 2 + k
                emit_unit(k, h, c, slot, value, (c >= 2) if first else (c >= 0))

            @pl.when(c > 0)
            def _():
                finish_unit(0, h, c - 1)
                finish_unit(1, h, c - 1)

            return 0

        lax.fori_loop(0, nc, body, 0)
        finish_unit(0, h, nc - 1)
        finish_unit(1, h, nc - 1)

    own_tok.wait()
    for copy in factors:
        copy.wait()
    low_of(gx)
    gate_up(gx, True)

    rb = 256

    def norm_chunk(pairs, wcols, a_t, count):
        def body(i, totals):
            rows = pl.ds(pl.multiple_of(i * rb, rb), rb)
            left = a_t[:, rows]
            out = []
            for (w, b), total in zip(pairs, totals):
                merged = w[rows, wcols].astype(F32) + contract_first(left, b)
                out.append(total + jnp.sum((merged * merged).reshape(rb // 8, 8, merged.shape[1]), axis=0))
            return tuple(out)

        zeros = tuple(jnp.zeros((8, b.shape[1]), F32) for _, b in pairs)
        totals = lax.fori_loop(0, count // rb, body, zeros)
        return [jnp.sum(total, axis=0, keepdims=True) for total in totals]

    def only(value, n):
        row = lax.broadcasted_iota(jnp.int32, value.shape, 0)
        keep = jnp.logical_and(row >= n * rank, row < (n + 1) * rank)
        return jnp.where(keep, value.astype(F32), 0.0).astype(BF16)

    def gate_norms(c, _):
        @pl.when(c + 2 < nc)
        def _():
            load_w(2, c + 2).start()

        b = deep[:, cols(c)]
        sums = norm_chunk(((wg, only(b, 0)), (wu, only(b, 1))), cols(c), wide, width)
        ngs[gy, 0:1, cols(c)] = sums[0]
        ngs[gy, 1:2, cols(c)] = sums[1]
        return 0

    lax.fori_loop(0, nc, gate_norms, 0)

    def ng_copy(i):
        peer = lax.rem(gy + i, 4)
        return remote(ngs.at[gy], ngs.at[gy], ng_send.at[i - 1], ng_recv.at[gy], {"gy": peer})

    for i in range(1, 4):
        ng_copy(i).start()

    pltpu.make_async_remote_copy(
        src_ref=tok_hbm, dst_ref=xt.at[1 - gx], send_sem=in_send.at[0], recv_sem=in_recv.at[0],
        device_id=y_peer, device_id_type=pl.DeviceIdType.MESH,
    ).wait_recv()
    low_of(1 - gx)
    gate_up(1 - gx, False)
    pl.semaphore_signal(credit.at[0], inc=1, device_id=core_peer, device_id_type=pl.DeviceIdType.MESH)

    place = gx * 4 + gz
    for c in range(nc):
        load_w(2, c).wait()

    def down_norms(t, _):
        sums = norm_chunk(((wd, only(wide[:, tile(t)], 2)),), tile(t), deep, hidden_l)
        nds[place, :, tile(t)] = sums[0]
        return 0

    lax.fori_loop(0, nt, down_norms, 0)

    def group_copy(buf, i, send, recv):
        peer, _ = group_peer(i)
        return remote(buf.at[place], buf.at[place], send.at[i - 1], recv.at[place], peer)

    def group_wait(buf, i, send, recv):
        peer, src = group_peer(i)
        remote(buf.at[src], buf.at[src], send.at[i - 1], recv.at[src], peer).wait_recv()

    for i in range(1, 8):
        group_copy(nds, i, nd_send, nd_recv.at[0]).start()
    for i in range(1, 8):
        group_wait(nds, i, nd_send, nd_recv.at[0])
    total = nds[0]
    for i in range(1, 8):
        total = total + nds[i]
    for i in range(width // LANES):
        part_cols = slice(i * LANES, (i + 1) * LANES)
        extra[1:2, part_cols] = m_d[i : i + 1]
    scale_d = extra[1:2, 0:width] / jnp.sqrt(total + EPSILON)
    own_cot.wait()
    pltpu.make_async_remote_copy(
        src_ref=cot_hbm, dst_ref=dl.at[1 - gx], send_sem=in_send.at[1], recv_sem=in_recv.at[1],
        device_id=y_peer, device_id_type=pl.DeviceIdType.MESH,
    ).wait_recv()
    for h in range(2):
        dl[h] = (dl[h].astype(F32) * scale_d).astype(BF16)

    def rows2(ref, *idx):
        value = ref[idx] if idx else ref[...]
        return value.reshape(2 * half_t, value.shape[-1])

    lane2 = lax.broadcasted_iota(jnp.int32, (2 * half_t, LANES), 1)
    is_down = jnp.logical_and(lane2 >= 2 * rank, lane2 < 3 * rank)
    down_back = jnp.where(is_down, contract_last(rows2(dl), wide[...]), 0.0)
    la[0] = (rows2(low) + down_back).astype(BF16)
    la_core = remote(la.at[0], lar.at[0], la_send.at[0], la_recv.at[0], core_peer)
    la_core.start()
    down_back = down_back.astype(BF16)

    def hidden_grads(c, _):
        value = contract_last(rows2(dl), wd[cols(c)]) + dot(down_back, deep[:, cols(c)])
        for h in range(2):
            slot = lax.rem(c, 2) * 2 + h
            emit_unit(2, h, c, slot, value[h * half_t : (h + 1) * half_t], c >= 0)

        @pl.when(c == 0)
        def _():
            la_core.wait_recv()
            la[1] = (la[0].astype(F32) + lar[0].astype(F32)).astype(BF16)
            remote(la.at[1], lar.at[1], la_send.at[1], la_recv.at[1], x_peer).start()

        @pl.when(c > 0)
        def _():
            finish_unit(2, 0, c - 1)
            finish_unit(2, 1, c - 1)

        return 0

    lax.fori_loop(0, nc, hidden_grads, 0)
    finish_unit(2, 0, nc - 1)
    finish_unit(2, 1, nc - 1)

    for i in range(1, 4):
        src = lax.rem(gy + i, 4)
        remote(ngs.at[src], ngs.at[src], ng_send.at[i - 1], ng_recv.at[src], {"gy": src}).wait_recv()
    for i in range(1, 4):
        ng_copy(i).wait_send()
    norm_gu = jnp.sqrt(ngs[0] + ngs[1] + ngs[2] + ngs[3] + EPSILON)
    scale_gu[0] = norm_gu
    for i in range(hidden_l // LANES):
        part_cols = slice(i * LANES, (i + 1) * LANES)
        for k in range(2):
            scale_gu[1, k : k + 1, part_cols] = m_gu[k, i : i + 1] / norm_gu[k : k + 1, part_cols]

    def ag_copy(k, buf, h, c):
        return remote(
            buf.at[h, mine, cols(c)], buf.at[h, mine, cols(c)],
            ag_send.at[unit_id(k, h, c)], ag_recv.at[unit_id(k, h, c)], core_peer,
        )

    def ag_wait(k, buf, h, c):
        remote(
            buf.at[h, other_rows, cols(c)], buf.at[h, other_rows, cols(c)],
            ag_send.at[unit_id(k, h, c)], ag_recv.at[unit_id(k, h, c)], core_peer,
        ).wait_recv()

    def lin(k, h, c):
        return part[k, h, mine, cols(c)].astype(F32) + xr[k, h, :, cols(c)].astype(F32)

    def hidden_of(h):
        def body(c, _):
            for k in range(2):
                x_copy(k, h, c).wait()
            gate_pre = lin(0, h, c) * scale_gu[1, 0:1, cols(c)]
            up_pre = lin(1, h, c) * scale_gu[1, 1:2, cols(c)]
            hid[h, mine, cols(c)] = (gate_pre * jax.nn.sigmoid(gate_pre) * up_pre).astype(BF16)
            ag_copy(2, hid, h, c).start()
            return 0

        lax.fori_loop(0, nc, body, 0)

    hidden_of(gx)
    hidden_of(1 - gx)

    def hidden_wait(c, _):
        for h in range(2):
            ag_wait(2, hid, h, c)
            ag_copy(2, hid, h, c).wait_send()
        return 0

    lax.fori_loop(0, nc, hidden_wait, 0)

    def low_chunk(c, total):
        return total + contract_last(rows2(hid, slice(None), slice(None), cols(c)), deep[:, cols(c)])

    down_low = lax.fori_loop(0, nc, low_chunk, jnp.zeros((2 * half_t, LANES), F32))
    down_low = jnp.where(is_down, down_low, 0.0)
    back[...] = down_low
    down_low = down_low.astype(BF16)

    sends = (
        (lambda t: (ysend.at[:, tile(t)], yrecv.at[:, tile(t)], y_peer)),
        (lambda t: (ykeep.at[pl.ds(pl.multiple_of((1 - bit0) * quarter, quarter), quarter), tile(t)], z1r.at[:, tile(t)], z1_peer)),
        (lambda t: (z1r.at[pl.ds(pl.multiple_of((1 - bit1) * (quarter // 2), quarter // 2), quarter // 2), tile(t)], z2r.at[:, tile(t)], z2_peer)),
    )
    kept1 = pl.ds(pl.multiple_of(bit0 * quarter, quarter), quarter)
    kept2 = pl.ds(pl.multiple_of(bit1 * (quarter // 2), quarter // 2), quarter // 2)
    peer_block = pl.ds(pl.multiple_of((bit0 * 2 + 1 - bit1) * (quarter // 2), quarter // 2), quarter // 2)
    gone1 = pl.ds(pl.multiple_of((1 - bit0) * quarter, quarter), quarter)

    def yz(v, s, t):
        if s < 3:
            src, dst, peer = sends[s](t)
        elif s == 3:
            src, dst, peer = obuf.at[my_rows, tile(t)], obuf.at[my_rows, tile(t)], z2_peer
        else:
            src, dst, peer = obuf.at[kept1, tile(t)], obuf.at[kept1, tile(t)], z1_peer
        return remote(src, dst, yz_send.at[v, s, t], yz_recv.at[v, s, t], peer)

    def yz_wait(v, s, t):
        if s < 3:
            yz(v, s, t).wait_recv()
        elif s == 3:
            remote(obuf.at[my_rows, tile(t)], obuf.at[peer_block, tile(t)], yz_send.at[v, s, t], yz_recv.at[v, s, t], z2_peer).wait_recv()
        else:
            remote(obuf.at[kept1, tile(t)], obuf.at[gone1, tile(t)], yz_send.at[v, s, t], yz_recv.at[v, s, t], z1_peer).wait_recv()

    def start_tile(v, t, value):
        for h in range(2):
            rows = value[h * half_t : (h + 1) * half_t].astype(BF16)

            @pl.when(h == gx)
            def _():
                ykeep[:, tile(t)] = rows

            @pl.when(h != gx)
            def _():
                ysend[:, tile(t)] = rows

        yz(v, 0, t).start()

    def yz_step(v, step):
        def at(s):
            t = step - s
            return t, jnp.logical_and(t >= 0, t < nt)

        t0, ok = at(0)

        @pl.when(ok)
        def _():
            yz_wait(v, 0, t0)
            total = ykeep[:, tile(t0)].astype(F32) + yrecv[:, tile(t0)].astype(F32)
            ykeep[:, tile(t0)] = total.astype(BF16)
            yz(v, 1, t0).start()

        t1, ok = at(1)

        @pl.when(ok)
        def _():
            yz_wait(v, 1, t1)
            total = ykeep[kept1, tile(t1)].astype(F32) + z1r[:, tile(t1)].astype(F32)
            z1r[:, tile(t1)] = total.astype(BF16)
            yz(v, 2, t1).start()

        t2, ok = at(2)

        @pl.when(ok)
        def _():
            yz_wait(v, 2, t2)
            total = z1r[kept2, tile(t2)].astype(F32) + z2r[:, tile(t2)].astype(F32)
            if v == 0:
                dots = cot_mine[:, tile(t2)].astype(F32) * total
                gds[place, :, tile(t2)] = jnp.sum(dots, axis=0, keepdims=True)
                total = total * scale_dv[:, tile(t2)]
            obuf[my_rows, tile(t2)] = total.astype(BF16)
            yz(v, 3, t2).start()

        t3, ok = at(3)

        @pl.when(ok)
        def _():
            yz_wait(v, 3, t3)
            yz(v, 4, t3).start()

        t4, ok = at(4)

        @pl.when(ok)
        def _():
            yz_wait(v, 4, t4)
            for s in range(5):
                yz(v, s, t4).wait_send()

    cot_rows.wait()
    scale_dv = extra.at[0:1, 0:width]
    scale_dv[...] = scale_d

    def down_tile(t, _):
        value = dot(rows2(hid), wd[:, tile(t)]) + dot(down_low, wide[:, tile(t)])
        start_tile(0, t, value)
        return 0

    lax.fori_loop(0, nt, down_tile, 0)

    acc[...] = jnp.zeros_like(acc)
    pl.semaphore_wait(credit.at[0], 1)

    def input_chunk(c):
        for h in range(2):
            ag_wait(0, part.at[0], h, c)
            ag_wait(1, part.at[1], h, c)
        gd = rows2(part, 0, slice(None), slice(None), cols(c))
        ud = rows2(part, 1, slice(None), slice(None), cols(c))

        def body(t, _):
            acc[:, tile(t)] += contract_last(gd, wg[tile(t), cols(c)]) + contract_last(ud, wu[tile(t), cols(c)])
            return 0

        lax.fori_loop(0, nt, body, 0)
        b = deep[:, cols(c)]
        pair = jnp.where(lane2 < rank, contract_last(gd, b), contract_last(ud, b))
        back[...] += jnp.where(lane2 < 2 * rank, pair, 0.0)

    def grads(c, _):
        sums = [None, None]
        for h in range(2):
            x_copy(2, h, c).wait()
            s_g, s_u = scale_gu[1, 0:1, cols(c)], scale_gu[1, 1:2, cols(c)]
            gate_lin, up_lin = lin(0, h, c), lin(1, h, c)
            hgrad = lin(2, h, c).astype(BF16).astype(F32)
            gate_pre, up_pre = gate_lin * s_g, up_lin * s_u
            sig = jax.nn.sigmoid(gate_pre)
            gate_grad = hgrad * up_pre * sig * (1.0 + gate_pre * (1.0 - sig))
            up_grad = hgrad * (gate_pre * sig)
            for k, value in ((0, gate_grad * gate_lin), (1, up_grad * up_lin)):
                piece = jnp.sum(value, axis=0, keepdims=True)
                sums[k] = piece if h == 0 else sums[k] + piece
            part[0, h, mine, cols(c)] = (gate_grad * s_g).astype(BF16)
            part[1, h, mine, cols(c)] = (up_grad * s_u).astype(BF16)
            ag_copy(0, part.at[0], h, c).start()
            ag_copy(1, part.at[1], h, c).start()
        gms[0:1, cols(c)] = sums[0]
        gms[1:2, cols(c)] = sums[1]

        @pl.when(c > 0)
        def _():
            input_chunk(c - 1)

        yz_step(0, c)
        return 0

    lax.fori_loop(0, nc, grads, 0)
    gm_core = remote(gms, gmr, gm_sem.at[0], gm_sem.at[1], core_peer)
    gm_core.start()
    input_chunk(nc - 1)

    def rest(step, _):
        yz_step(0, step)
        return 0

    lax.fori_loop(nc, max(nc, nt + 4), rest, 0)
    for n, peer in ((1, y_peer), (2, z1_peer), (3, z2_peer)):
        pl.semaphore_signal(credit.at[n], inc=1, device_id=peer, device_id_type=pl.DeviceIdType.MESH)
    for i in range(1, 8):
        group_copy(gds, i, gd_send, nd_recv.at[1]).start()
    for n in range(1, 4):
        pl.semaphore_wait(credit.at[n], 1)
    out_copy = pltpu.make_async_copy(obuf, out_hbm, out_sem.at[0])
    out_copy.start()

    back_gu = jnp.where(lane2 < 2 * rank, back[...], 0.0).astype(BF16)
    lb[0] = back[...].astype(BF16)

    def input_tile(t, _):
        start_tile(1, t, acc[:, tile(t)] + dot(back_gu, wide[:, tile(t)]))
        return 0

    lax.fori_loop(0, nt, input_tile, 0)
    lb_peers = (y_peer, z1_peer, z2_peer)

    def lb_copy(n):
        return remote(lb.at[n], lbr.at[n], lb_send.at[n], lb_recv.at[n], lb_peers[n])

    lb_copy(0).start()
    out_copy.wait()

    def last(step, _):
        yz_step(1, step)
        for n in range(3):

            @pl.when(step == nt - 1 + n)
            def _():
                lb_copy(n).wait()
                lb[n + 1] = (lb[n].astype(F32) + lbr[n].astype(F32)).astype(BF16)
                if n < 2:
                    lb_copy(n + 1).start()

        return 0

    lax.fori_loop(0, nt + 4, last, 0)
    gtok_copy = pltpu.make_async_copy(obuf, gtok_hbm, out_sem.at[1])
    gtok_copy.start()

    gm_core.wait()
    gms[...] = (gms[...] + gmr[...]) / scale_gu[0]
    for i in range(hidden_l // LANES):
        for k in range(2):
            gm_out[k, i : i + 1] = gms[k : k + 1, i * LANES : (i + 1) * LANES]
    ends = [
        pltpu.make_async_copy(gm_out.at[0], gmg_hbm, out_sem.at[2]),
        pltpu.make_async_copy(gm_out.at[1], gmu_hbm, out_sem.at[3]),
    ]
    for i in range(1, 8):
        group_wait(gds, i, gd_send, nd_recv.at[1])
    for i in range(1, 8):
        group_copy(gds, i, gd_send, nd_recv.at[1]).wait_send()
        group_copy(nds, i, nd_send, nd_recv.at[0]).wait_send()
    total, norm = gds[0], nds[0]
    for i in range(1, 8):
        total, norm = total + gds[i], norm + nds[i]
    total = total / jnp.sqrt(norm + EPSILON)
    for i in range(width // LANES):
        gd_out[i : i + 1] = total[:, i * LANES : (i + 1) * LANES]
    ends.append(pltpu.make_async_copy(gd_out, gdm_hbm, out_sem.at[4]))
    for copy in ends:
        copy.start()

    la_core.wait_send()
    remote(la.at[1], lar.at[1], la_send.at[1], la_recv.at[1], x_peer).wait()
    la_t = (la[1].astype(F32) + lar[1].astype(F32)).T.astype(BF16)
    lb_t = lb[3].astype(F32).T.astype(BF16)
    acc[0 : 2 * rank] = dot(lb_t[: 2 * rank], rows2(xt))
    acc[2 * rank : 3 * rank] = dot(lb_t[2 * rank : 3 * rank], rows2(dl))
    for n, dst in enumerate((grg_hbm, gru_hbm, gde_hbm)):
        ends.append(pltpu.make_async_copy(acc.at[n * rank : (n + 1) * rank], dst, out_sem.at[5 + n]))
        ends[-1].start()
    cut = hidden_l // 2
    expand_outs = (geg_hbm, geu_hbm, gdr_hbm)
    for k in range(3):
        rows = la_t[k * rank : (k + 1) * rank]
        for j in range(2):
            piece = pl.ds(j * cut, cut)
            if k < 2:
                right = rows2(part, k, slice(None), slice(None), piece)
            else:
                right = rows2(hid, slice(None), slice(None), piece)
            n = k * 2 + j
            if n < 5:
                where = acc.at[(3 + n) * rank : (4 + n) * rank, 0:cut]
            else:
                where = extra.at[:, 0:cut]
            where[...] = dot(rows, right)
            ends.append(pltpu.make_async_copy(where, expand_outs[k].at[:, piece], out_sem.at[8 + n]))
            ends[-1].start()
    for copy in ends + [gtok_copy]:
        copy.wait()

    send_tok.wait_send()
    send_cot.wait_send()
    for slot in range(4):
        core_copy(2, slot % 2, nc - 1, slot).wait_send()

    def ag_sends(c, _):
        for h in range(2):
            ag_copy(0, part.at[0], h, c).wait_send()
            ag_copy(1, part.at[1], h, c).wait_send()
        return 0

    lax.fori_loop(0, nc, ag_sends, 0)


def hand_over(*refs):
    sources, targets, sem = refs[:11], refs[11:22], refs[22]
    copies = [pltpu.make_async_copy(sources[i], targets[i], sem.at[i]) for i in range(11)]
    for copy in copies:
        copy.start()
    for copy in copies:
        copy.wait()


def fits(tokens, gate_weight, gate_expand):
    half_t, width = tokens.shape
    hidden_l, rank = gate_weight.shape[1], gate_expand.shape[0]
    sizes = tuple(lax.axis_size(name) for name in ("gx", "gy", "gz"))
    return (
        sizes == (2, 4, 4)
        and 3 * rank <= LANES
        and rank % 16 == 0
        and half_t % 128 == 0
        and width % LANES == 0
        and 2 * half_t >= 8 * rank
        and width % 256 == 0
        and hidden_l % 512 == 0
        and hidden_l % 256 == 0
        and hidden_l >= 1024
        and hidden_l // 2 <= width
        and 6 * width * hidden_l <= 45 * 2**20
        and half_t * width <= 2**18
    )


def fused(
    tokens, cotangent, gate_weight, up_weight, down_weight, gate_reduce, gate_expand,
    gate_magnitude, up_reduce, up_expand, up_magnitude, down_reduce, down_expand, down_magnitude,
):
    half_t, width = tokens.shape
    hidden_l, rank = gate_weight.shape[1], gate_expand.shape[0]
    all_t, quarter = 2 * half_t, half_t // 2
    fc, dt = 512, 512 if width % 512 == 0 else width
    nc, nt = hidden_l // fc, width // dt
    any_space = pl.BlockSpec(memory_space=pl.ANY)
    dma = pltpu.SemaphoreType.DMA
    units = 6 * nc
    rows_f, rows_d = hidden_l // LANES, width // LANES
    shapes = (
        ((half_t, width), BF16), ((half_t, width), BF16),
        ((rank, width), F32), ((rank, width), F32), ((rank, width), F32),
        ((rank, hidden_l), F32), ((rank, hidden_l), F32), ((rank, hidden_l), F32),
        ((rows_f, LANES), F32), ((rows_f, LANES), F32), ((rows_d, LANES), F32),
    )
    results = pl.pallas_call(
        kernel,
        out_shape=[jax.ShapeDtypeStruct(*pair) for pair in shapes],
        in_specs=[any_space] * 14,
        out_specs=[any_space] * 11,
        scratch_shapes=[
            pltpu.VMEM((LANES, width), BF16),
            pltpu.VMEM((LANES, hidden_l), BF16),
            pltpu.VMEM((2, rows_f, LANES), F32),
            pltpu.VMEM((rows_d, LANES), F32),
            pltpu.VMEM((2, rows_f, LANES), F32),
            pltpu.VMEM((rows_d, LANES), F32),
            pltpu.VMEM((width, hidden_l), BF16),
            pltpu.VMEM((width, hidden_l), BF16),
            pltpu.VMEM((hidden_l, width), BF16),
            pltpu.VMEM((2, half_t, width), BF16),
            pltpu.VMEM((2, half_t, width), BF16),
            pltpu.VMEM((3, 2, half_t, hidden_l), BF16),
            pltpu.VMEM((3, 2, quarter, hidden_l), BF16),
            pltpu.VMEM((2, half_t, hidden_l), BF16),
            pltpu.VMEM((4, quarter, fc), BF16),
            pltpu.VMEM((all_t, width), F32),
            pltpu.VMEM((half_t, width), BF16),
            pltpu.VMEM((half_t, width), BF16),
            pltpu.VMEM((half_t, width), BF16),
            pltpu.VMEM((quarter, width), BF16),
            pltpu.VMEM((quarter // 2, width), BF16),
            pltpu.VMEM((half_t, width), BF16),
            pltpu.VMEM((half_t // 4, width), BF16),
            pltpu.VMEM((2, half_t, LANES), F32),
            pltpu.VMEM((2, all_t, LANES), BF16),
            pltpu.VMEM((2, all_t, LANES), BF16),
            pltpu.VMEM((all_t, LANES), F32),
            pltpu.VMEM((4, all_t, LANES), BF16),
            pltpu.VMEM((3, all_t, LANES), BF16),
            pltpu.VMEM((8, 1, width), F32),
            pltpu.VMEM((4, 2, hidden_l), F32),
            pltpu.VMEM((2, 2, hidden_l), F32),
            pltpu.VMEM((2, hidden_l), F32),
            pltpu.VMEM((2, hidden_l), F32),
            pltpu.VMEM((8, 1, width), F32),
            pltpu.VMEM((rank, width), F32),
            dma((3, nc)),
            dma((12,)),
            dma((2,)),
            dma((2,)),
            dma((4,)),
            dma((units,)),
            dma((units,)),
            dma((units,)),
            dma((units,)),
            dma((units,)),
            dma((2, 5, nt)),
            dma((2, 5, nt)),
            dma((7,)),
            dma((7,)),
            dma((2, 8)),
            dma((3,)),
            dma((4,)),
            dma((2,)),
            dma((2,)),
            dma((3,)),
            dma((3,)),
            dma((2,)),
            dma((14,)),
            pltpu.SemaphoreType.REGULAR((4,)),
        ],
        compiler_params=pltpu.CompilerParams(
            collective_id=0, has_side_effects=True, vmem_limit_bytes=67043328
        ),
    )(
        tokens, cotangent, gate_weight, up_weight, down_weight, gate_reduce.T, up_reduce.T,
        down_expand, gate_expand, up_expand, down_reduce.T, gate_magnitude.reshape(rows_f, LANES),
        up_magnitude.reshape(rows_f, LANES), down_magnitude.reshape(rows_d, LANES),
    )
    results = pl.pallas_call(
        hand_over,
        out_shape=[jax.ShapeDtypeStruct(*pair) for pair in shapes],
        in_specs=[pl.BlockSpec(memory_space=pltpu.VMEM)] * 11,
        out_specs=[any_space] * 11,
        scratch_shapes=[dma((11,))],
        compiler_params=pltpu.CompilerParams(vmem_limit_bytes=2**23),
    )(*results)
    output, grad_tokens, grg, gru, gde, geg, geu, gdr, gmg, gmu, gdm = results
    return (
        output, grad_tokens, grg.T, geg, gmg.reshape(-1), gru.T, geu, gmu.reshape(-1),
        gdr.T, gde, gdm.reshape(-1),
    )


def choose_body(mesh):
    def body(*args):
        if fits(args[0], args[2], args[6]):
            return fused(*args)
        return on_device(*args)

    return body


def solution(mesh):
    return jax.shard_map(
        choose_body(mesh),
        mesh=mesh,
        in_specs=(
            P("gx", "gy"),
            P("gx", "gy"),
            P("gy", ("gx", "gz")),
            P("gy", ("gx", "gz")),
            P(("gx", "gz"), "gy"),
            P("gy", None),
            P(None, ("gx", "gz")),
            P(("gx", "gz")),
            P("gy", None),
            P(None, ("gx", "gz")),
            P(("gx", "gz")),
            P(("gx", "gz"), None),
            P(None, "gy"),
            P("gy"),
        ),
        out_specs=(
            P("gx", "gy"),
            P("gx", "gy"),
            P("gy", None),
            P(None, ("gx", "gz")),
            P(("gx", "gz")),
            P("gy", None),
            P(None, ("gx", "gz")),
            P(("gx", "gz")),
            P(("gx", "gz"), None),
            P(None, "gy"),
            P("gy"),
        ),
        check_vma=False,
    )
```

```python
import functools

import jax
import jax.numpy as jnp
from jax import lax
from jax.experimental import pallas as pl
from jax.experimental.pallas import tpu as pltpu
from jax.sharding import PartitionSpec as P

EPSILON = 1e-06
BF16 = jnp.bfloat16
F32 = jnp.float32


def tile_square(weight, reduce_in, expand_out):
    merged = weight.astype(jnp.float32) + jnp.dot(
        reduce_in, expand_out, preferred_element_type=jnp.float32
    )
    return jnp.sum(merged * merged, axis=0)


def share_rows(values, count):
    return lax.dynamic_slice_in_dim(values, lax.axis_index("gz") * count, count, 0)


def contract_last(left, right):
    return lax.dot_general(
        left, right, (((1,), (1,)), ((), ())), preferred_element_type=jnp.float32
    )


def contract_first(left, right):
    return lax.dot_general(
        left, right, (((0,), (0,)), ((), ())), preferred_element_type=jnp.float32
    )


def scatter_pair(part, low_part, axes):
    width = part.shape[1]
    joined = jnp.concatenate(
        [part.astype(jnp.bfloat16), low_part.astype(jnp.bfloat16)], axis=1
    )
    summed = lax.psum_scatter(joined, axes, scatter_dimension=0, tiled=True)
    return summed[:, :width].astype(jnp.float32), summed[:, width:]


def on_device(
    tokens,
    cotangent,
    gate_weight,
    up_weight,
    down_weight,
    gate_reduce,
    gate_expand,
    gate_magnitude,
    up_reduce,
    up_expand,
    up_magnitude,
    down_reduce,
    down_expand,
    down_magnitude,
):
    share_count = tokens.shape[0] // lax.axis_size("gz")
    square_gate = tile_square(gate_weight, gate_reduce, gate_expand)
    square_up = tile_square(up_weight, up_reduce, up_expand)
    square_down = tile_square(down_weight, down_reduce, down_expand)
    norm_down = jnp.sqrt(lax.psum(square_down, ("gx", "gz")) + EPSILON)
    scale_down = down_magnitude / norm_down
    all_tokens = lax.all_gather(tokens, "gx", axis=0, tiled=True)
    part_gate = jnp.dot(all_tokens, gate_weight, preferred_element_type=jnp.float32)
    part_up = jnp.dot(all_tokens, up_weight, preferred_element_type=jnp.float32)
    low_gate_part = jnp.dot(all_tokens, gate_reduce, preferred_element_type=jnp.float32)
    low_up_part = jnp.dot(all_tokens, up_reduce, preferred_element_type=jnp.float32)
    gate_lin, gate_low = scatter_pair(part_gate, low_gate_part, "gy")
    up_lin, up_low = scatter_pair(part_up, low_up_part, "gy")
    summed_gate, summed_up = lax.psum((square_gate, square_up), "gy")
    norm_gate = jnp.sqrt(summed_gate + EPSILON)
    norm_up = jnp.sqrt(summed_up + EPSILON)
    scale_gate = gate_magnitude / norm_gate
    scale_up = up_magnitude / norm_up
    gate_lin = gate_lin + jnp.dot(gate_low, gate_expand, preferred_element_type=jnp.float32)
    up_lin = up_lin + jnp.dot(up_low, up_expand, preferred_element_type=jnp.float32)
    gate_pre = gate_lin * scale_gate[None, :]
    up_pre = up_lin * scale_up[None, :]
    sigmoid_gate = jax.nn.sigmoid(gate_pre)
    active = gate_pre * sigmoid_gate
    hidden = (active * up_pre).astype(jnp.bfloat16)
    all_hidden = lax.all_gather(hidden, "gy", axis=0, tiled=True)
    part_down = jnp.dot(all_hidden, down_weight, preferred_element_type=jnp.float32)
    low_down_part = jnp.dot(all_hidden, down_reduce, preferred_element_type=jnp.float32)
    down_lin, down_low = scatter_pair(part_down, low_down_part, ("gx", "gz"))
    down_lin = down_lin + jnp.dot(down_low, down_expand, preferred_element_type=jnp.float32)
    output = lax.all_gather(
        (down_lin * scale_down[None, :]).astype(jnp.bfloat16), "gz", axis=0, tiled=True
    )
    cot_float = cotangent.astype(jnp.float32)
    down_delta = (cot_float * scale_down[None, :]).astype(jnp.bfloat16)
    cot_share = share_rows(cot_float, share_count)
    delta_share = share_rows(down_delta, share_count)
    grad_down_magnitude = jnp.sum(cot_share * down_lin, axis=0) / norm_down
    grad_down_expand = contract_first(down_low, delta_share)
    grad_down_magnitude, grad_down_expand = lax.psum(
        (grad_down_magnitude, grad_down_expand), ("gx", "gz")
    )
    all_delta = lax.all_gather(down_delta, "gx", axis=0, tiled=True)
    part_hidden_grad = contract_last(all_delta, down_weight)
    part_down_back = contract_last(all_delta, down_expand)
    hidden_gradsum, down_back = scatter_pair(part_hidden_grad, part_down_back, "gy")
    hidden_grad = (hidden_gradsum + contract_last(down_back, down_reduce)).astype(jnp.bfloat16)
    hgrad_float = hidden_grad.astype(jnp.float32)
    gate_grad = hgrad_float * up_pre * sigmoid_gate * (1.0 + gate_pre * (1.0 - sigmoid_gate))
    up_grad = hgrad_float * active
    gate_delta = (gate_grad * scale_gate[None, :]).astype(jnp.bfloat16)
    up_delta = (up_grad * scale_up[None, :]).astype(jnp.bfloat16)
    grad_gate_magnitude = jnp.sum(gate_grad * gate_lin, axis=0) / norm_gate
    grad_up_magnitude = jnp.sum(up_grad * up_lin, axis=0) / norm_up
    grad_gate_magnitude, grad_up_magnitude = lax.psum(
        (grad_gate_magnitude, grad_up_magnitude), "gy"
    )
    rank = gate_low.shape[1]
    all_low = lax.all_gather(
        jnp.concatenate([gate_low, up_low, down_back], axis=1), "gy", axis=0, tiled=True
    )
    all_gate_delta, all_up_delta = (
        lax.all_gather(gate_delta, "gy", axis=0, tiled=True),
        lax.all_gather(up_delta, "gy", axis=0, tiled=True),
    )
    grad_gate_expand = contract_first(all_low[:, :rank], all_gate_delta)
    grad_up_expand = contract_first(all_low[:, rank : 2 * rank], all_up_delta)
    grad_down_reduce = contract_first(all_hidden, all_low[:, 2 * rank :])
    part_input = contract_last(all_gate_delta, gate_weight) + contract_last(all_up_delta, up_weight)
    part_gate_back = contract_last(all_gate_delta, gate_expand)
    part_up_back = contract_last(all_up_delta, up_expand)
    input_sum, back_pair = scatter_pair(
        part_input, jnp.concatenate([part_gate_back, part_up_back], axis=1), ("gx", "gz")
    )
    gate_back = back_pair[:, :rank]
    up_back = back_pair[:, rank:]
    grad_tokens = lax.all_gather(
        (
            input_sum + contract_last(gate_back, gate_reduce) + contract_last(up_back, up_reduce)
        ).astype(jnp.bfloat16),
        "gz",
        axis=0,
        tiled=True,
    )
    token_share = share_rows(tokens, share_count)
    grad_gate_reduce = contract_first(token_share, gate_back)
    grad_up_reduce = contract_first(token_share, up_back)
    grad_gate_reduce, grad_up_reduce = lax.psum((grad_gate_reduce, grad_up_reduce), ("gx", "gz"))
    return (
        output,
        grad_tokens,
        grad_gate_reduce,
        grad_gate_expand,
        grad_gate_magnitude,
        grad_up_reduce,
        grad_up_expand,
        grad_up_magnitude,
        grad_down_reduce,
        grad_down_expand,
        grad_down_magnitude,
    )


LANES = 128


def dot(left, right):
    return jnp.dot(left, right, preferred_element_type=F32)


def kernel(
    tok_hbm, cot_hbm, wg_hbm, wu_hbm, wd_hbm, ag_hbm, au_hbm, bd_hbm, bg_hbm, bu_hbm, ad_hbm,
    mg_hbm, mu_hbm, md_hbm,
    out_hbm, gtok_hbm, grg_hbm, gru_hbm, gde_hbm, geg_hbm, geu_hbm, gdr_hbm,
    gmg_hbm, gmu_hbm, gdm_hbm,
    wide, deep, m_gu, m_d, gm_out, gd_out,
    wg, wu, wd, xt, dl, part, xr, hid, cs, acc, ysend, ykeep, yrecv, z1r, z2r,
    obuf, cot_mine, low, la, lar, back, lb, lbr, nds, ngs, scale_gu, gms, gmr, gds, extra,
    w_sem, in_sem, in_send, in_recv, cs_sem, c_recv, x_send, x_recv, ag_send, ag_recv,
    yz_send, yz_recv, nd_send, gd_send, nd_recv, ng_send, ng_recv, la_send, la_recv,
    lb_send, lb_recv, gm_sem, out_sem, credit,
):
    gx, gy, gz = lax.axis_index("gx"), lax.axis_index("gy"), lax.axis_index("gz")
    core = lax.rem(gy, 2)
    bit0, bit1 = lax.rem(gz, 2), gz // 2
    core_peer = {"gy": gy + 1 - 2 * core}
    x_peer = {"gy": lax.rem(gy + 2, 4)}
    y_peer = {"gx": 1 - gx}
    z1_peer = {"gz": gz + 1 - 2 * bit0}
    z2_peer = {"gz": lax.rem(gz + 2, 4)}
    half_t, width = xt.shape[1], xt.shape[2]
    quarter = half_t // 2
    hidden_l = wg.shape[1]
    rank = gde_hbm.shape[0]
    fc = cs.shape[2]
    nc = hidden_l // fc
    dt = 256
    nt = width // dt
    mine = pl.ds(pl.multiple_of(core * quarter, quarter), quarter)

    def cols(c):
        return pl.ds(pl.multiple_of(c * fc, fc), fc)

    def tile(t):
        return pl.ds(pl.multiple_of(t * dt, dt), dt)

    def remote(src, dst, send, recv, peer):
        return pltpu.make_async_remote_copy(
            src_ref=src, dst_ref=dst, send_sem=send, recv_sem=recv,
            device_id=peer, device_id_type=pl.DeviceIdType.MESH,
        )

    def group_peer(i):
        place = lax.rem(gx * 4 + gz + i, 8)
        return {"gx": place // 4, "gz": lax.rem(place, 4)}, place

    barrier = pltpu.get_barrier_semaphore()
    for i in range(1, 4):
        pl.semaphore_signal(barrier, inc=1, device_id={"gy": lax.rem(gy + i, 4)}, device_id_type=pl.DeviceIdType.MESH)
    for i in range(1, 8):
        pl.semaphore_signal(barrier, inc=1, device_id=group_peer(i)[0], device_id_type=pl.DeviceIdType.MESH)

    own_tok = pltpu.make_async_copy(tok_hbm, xt.at[gx], in_sem.at[0])
    own_cot = pltpu.make_async_copy(cot_hbm, dl.at[gx], in_sem.at[1])
    block = (bit0 * 2 + bit1) * (half_t // 4)
    my_rows = pl.ds(pl.multiple_of(block, half_t // 4), half_t // 4)
    cot_rows = pltpu.make_async_copy(cot_hbm.at[my_rows], cot_mine, in_sem.at[2])
    own_tok.start()
    factors = [
        pltpu.make_async_copy(src, buf.at[n * rank : (n + 1) * rank], in_sem.at[3 + i])
        for i, (src, buf, n) in enumerate((
            (ag_hbm, wide, 0), (au_hbm, wide, 1), (bg_hbm, deep, 0), (bu_hbm, deep, 1),
            (bd_hbm, wide, 2), (ad_hbm, deep, 2),
        ))
    ]
    factors += [
        pltpu.make_async_copy(src, dst, in_sem.at[9 + i])
        for i, (src, dst) in enumerate(((mg_hbm, m_gu.at[0]), (mu_hbm, m_gu.at[1]), (md_hbm, m_d)))
    ]
    for copy in factors[:4]:
        copy.start()

    def load_w(k, c):
        if k == 0:
            return pltpu.make_async_copy(wg_hbm.at[:, cols(c)], wg.at[:, cols(c)], w_sem.at[0, c])
        if k == 1:
            return pltpu.make_async_copy(wu_hbm.at[:, cols(c)], wu.at[:, cols(c)], w_sem.at[1, c])
        return pltpu.make_async_copy(wd_hbm.at[cols(c)], wd.at[cols(c)], w_sem.at[2, c])

    for c in range(2):
        load_w(0, c).start()
        load_w(1, c).start()
    for copy in factors[4:]:
        copy.start()
    wide[3 * rank :] = jnp.zeros((wide.shape[0] - 3 * rank, width), BF16)
    deep[3 * rank :] = jnp.zeros((deep.shape[0] - 3 * rank, hidden_l), BF16)
    pl.semaphore_wait(barrier, 10)
    send_tok = remote(tok_hbm, xt.at[gx], in_send.at[0], in_recv.at[0], y_peer)
    send_cot = remote(cot_hbm, dl.at[gx], in_send.at[1], in_recv.at[1], y_peer)
    send_tok.start()
    own_cot.start()
    cot_rows.start()

    lane = lax.broadcasted_iota(jnp.int32, (half_t, low.shape[2]), 1)
    is_gate = lane < rank

    def low_of(h):
        low[h] = jnp.where(lane < 2 * rank, contract_last(xt[h], wide[...]), 0.0)

    def unit_id(k, h, c):
        return (k * 2 + h) * nc + c

    def core_copy(k, h, c, slot):
        return remote(
            cs.at[slot], part.at[k, h, mine, cols(c)], cs_sem.at[slot],
            c_recv.at[unit_id(k, h, c)], core_peer,
        )

    other_rows = pl.ds(pl.multiple_of((1 - core) * quarter, quarter), quarter)

    def x_copy(k, h, c):
        return remote(
            part.at[k, h, mine, cols(c)], xr.at[k, h, :, cols(c)],
            x_send.at[unit_id(k, h, c)], x_recv.at[unit_id(k, h, c)], x_peer,
        )

    def emit_unit(k, h, c, slot, value, reuse):
        lo, hi = value[:quarter], value[quarter:]
        part[k, h, mine, cols(c)] = jnp.where(core == 0, lo, hi).astype(BF16)

        @pl.when(reuse)
        def _():
            core_copy(k, h, c, slot).wait_send()

        cs[slot] = jnp.where(core == 0, hi, lo).astype(BF16)
        core_copy(k, h, c, slot).start()

    def finish_unit(k, h, c):
        pltpu.make_async_remote_copy(
            src_ref=cs.at[0], dst_ref=part.at[k, h, other_rows, cols(c)], send_sem=cs_sem.at[0],
            recv_sem=c_recv.at[unit_id(k, h, c)], device_id=core_peer,
            device_id_type=pl.DeviceIdType.MESH,
        ).wait_recv()
        total = part[k, h, mine, cols(c)].astype(F32) + part[k, h, other_rows, cols(c)].astype(F32)
        part[k, h, mine, cols(c)] = total.astype(BF16)
        x_copy(k, h, c).start()

    rb = 256

    def squares(w, wcols, count):
        total = None
        for i in range(count // rb):
            piece = w[i * rb : (i + 1) * rb, wcols].astype(F32)
            piece = jnp.sum((piece * piece).reshape(rb // 8, 8, piece.shape[1]), axis=0)
            total = piece if total is None else total + piece
        return jnp.sum(total, axis=0, keepdims=True)

    def fold(factor, cross, spread):
        return jnp.sum(factor * (2.0 * cross + spread), axis=0, keepdims=True)

    def gate_up(h, first):
        x_low = low[h]
        low_gate = jnp.where(is_gate, x_low, 0.0).astype(BF16)
        low_up = jnp.where(is_gate, 0.0, x_low).astype(BF16)

        def body(c, _):
            if first:
                load_w(0, c).wait()
                load_w(1, c).wait()

                @pl.when(c + 2 < nc)
                def _():
                    load_w(0, c + 2).start()
                    load_w(1, c + 2).start()

                @pl.when(c + 2 >= nc)
                def _():
                    load_w(2, c + 2 - nc).start()

            if first:
                factor = deep[0 : 2 * rank, cols(c)]
                spread = dot(gram_hi, factor) + dot(gram_lo, factor)
                factor = factor.astype(F32)
            for k, w, lw in ((0, wg, low_gate), (1, wu, low_up)):
                extra_value = dot(lw, deep[:, cols(c)])
                if first:
                    left = jnp.concatenate([xt[h], wide[0 : 2 * rank]], axis=0)
                    both = dot(left, w[:, cols(c)])
                    value = both[:half_t] + extra_value
                    mine_rows = slice(k * rank, (k + 1) * rank)
                    ngs[gy, k : k + 1, cols(c)] = squares(w, cols(c), width) + fold(
                        factor[mine_rows], both[half_t:][mine_rows], spread[mine_rows]
                    )
                else:
                    value = dot(xt[h], w[:, cols(c)]) + extra_value
                slot = lax.rem(c, 2) * 2 + k
                emit_unit(k, h, c, slot, value, (c >= 2) if first else (c >= 0))

            @pl.when(c > 0)
            def _():
                finish_unit(0, h, c - 1)
                finish_unit(1, h, c - 1)

            return 0

        lax.fori_loop(0, nc, body, 0)
        finish_unit(0, h, nc - 1)
        finish_unit(1, h, nc - 1)

    own_tok.wait()
    for copy in factors:
        copy.wait()
    low_of(gx)
    gram = contract_last(wide[0 : 2 * rank], wide[0 : 2 * rank])
    side = lax.broadcasted_iota(jnp.int32, gram.shape, 0) < rank
    side = side == (lax.broadcasted_iota(jnp.int32, gram.shape, 1) < rank)
    gram = jnp.where(side, gram, 0.0)
    gram_hi = gram.astype(BF16)
    gram_lo = (gram - gram_hi.astype(F32)).astype(BF16)
    gate_up(gx, True)

    for c in range(2, nc):
        load_w(2, c).start()

    def ng_copy(i):
        peer = lax.rem(gy + i, 4)
        return remote(ngs.at[gy], ngs.at[gy], ng_send.at[i - 1], ng_recv.at[gy], {"gy": peer})

    for i in range(1, 4):
        ng_copy(i).start()

    send_tok.wait_send()
    send_cot.start()

    place = gx * 4 + gz
    for c in range(nc):
        load_w(2, c).wait()

    down_in = slice(2 * rank, 3 * rank)
    gram_d = contract_last(deep[down_in], deep[down_in])
    gram_d_hi = gram_d.astype(BF16)
    gram_d_lo = (gram_d - gram_d_hi.astype(F32)).astype(BF16)

    def down_norms(t, _):
        factor = wide[down_in, tile(t)]
        spread = dot(gram_d_hi, factor) + dot(gram_d_lo, factor)
        cross = dot(deep[down_in], wd[:, tile(t)])
        nds[place, :, tile(t)] = squares(wd, tile(t), hidden_l) + fold(factor.astype(F32), cross, spread)
        return 0

    lax.fori_loop(0, nt, down_norms, 0)

    def group_copy(buf, i, send, recv):
        peer, _ = group_peer(i)
        return remote(buf.at[place], buf.at[place], send.at[i - 1], recv.at[place], peer)

    def group_wait(buf, i, send, recv):
        peer, src = group_peer(i)
        remote(buf.at[src], buf.at[src], send.at[i - 1], recv.at[src], peer).wait_recv()

    for i in range(1, 8):
        group_copy(nds, i, nd_send, nd_recv.at[0]).start()
    pltpu.make_async_remote_copy(
        src_ref=tok_hbm, dst_ref=xt.at[1 - gx], send_sem=in_send.at[0], recv_sem=in_recv.at[0],
        device_id=y_peer, device_id_type=pl.DeviceIdType.MESH,
    ).wait_recv()
    low_of(1 - gx)
    gate_up(1 - gx, False)
    pl.semaphore_signal(credit.at[0], inc=1, device_id=core_peer, device_id_type=pl.DeviceIdType.MESH)

    for i in range(1, 8):
        group_wait(nds, i, nd_send, nd_recv.at[0])
    total = nds[0]
    for i in range(1, 8):
        total = total + nds[i]
    for i in range(width // LANES):
        part_cols = slice(i * LANES, (i + 1) * LANES)
        extra[1:2, part_cols] = m_d[i : i + 1]
    scale_d = extra[1:2, 0:width] / jnp.sqrt(jnp.maximum(total, 0.0) + EPSILON)
    own_cot.wait()
    pltpu.make_async_remote_copy(
        src_ref=cot_hbm, dst_ref=dl.at[1 - gx], send_sem=in_send.at[1], recv_sem=in_recv.at[1],
        device_id=y_peer, device_id_type=pl.DeviceIdType.MESH,
    ).wait_recv()
    for h in range(2):
        dl[h] = (dl[h].astype(F32) * scale_d).astype(BF16)

    def rows2(ref, *idx):
        value = ref[idx] if idx else ref[...]
        return value.reshape(2 * half_t, value.shape[-1])

    lane2 = lax.broadcasted_iota(jnp.int32, (2 * half_t, LANES), 1)
    is_down = jnp.logical_and(lane2 >= 2 * rank, lane2 < 3 * rank)
    down_back = jnp.where(is_down, contract_last(rows2(dl), wide[...]), 0.0)
    la[0] = (rows2(low) + down_back).astype(BF16)
    la_core = remote(la.at[0], lar.at[0], la_send.at[0], la_recv.at[0], core_peer)
    la_core.start()
    down_back = down_back.astype(BF16)

    def hidden_grads(c, _):
        value = contract_last(rows2(dl), wd[cols(c)]) + dot(down_back, deep[:, cols(c)])
        for h in range(2):
            slot = lax.rem(c, 2) * 2 + h
            emit_unit(2, h, c, slot, value[h * half_t : (h + 1) * half_t], c >= 0)

        @pl.when(c == 0)
        def _():
            la_core.wait_recv()
            la[1] = (la[0].astype(F32) + lar[0].astype(F32)).astype(BF16)
            remote(la.at[1], lar.at[1], la_send.at[1], la_recv.at[1], x_peer).start()

        @pl.when(c > 0)
        def _():
            finish_unit(2, 0, c - 1)
            finish_unit(2, 1, c - 1)

        return 0

    lax.fori_loop(0, nc, hidden_grads, 0)
    finish_unit(2, 0, nc - 1)
    finish_unit(2, 1, nc - 1)

    for i in range(1, 4):
        src = lax.rem(gy + i, 4)
        remote(ngs.at[src], ngs.at[src], ng_send.at[i - 1], ng_recv.at[src], {"gy": src}).wait_recv()
    for i in range(1, 4):
        ng_copy(i).wait_send()
    norm_gu = jnp.sqrt(jnp.maximum(ngs[0] + ngs[1] + ngs[2] + ngs[3], 0.0) + EPSILON)
    scale_gu[0] = norm_gu
    for i in range(hidden_l // LANES):
        part_cols = slice(i * LANES, (i + 1) * LANES)
        for k in range(2):
            scale_gu[1, k : k + 1, part_cols] = m_gu[k, i : i + 1] / norm_gu[k : k + 1, part_cols]

    def ag_copy(k, buf, h, c):
        return remote(
            buf.at[h, mine, cols(c)], buf.at[h, mine, cols(c)],
            ag_send.at[unit_id(k, h, c)], ag_recv.at[unit_id(k, h, c)], core_peer,
        )

    def ag_wait(k, buf, h, c):
        remote(
            buf.at[h, other_rows, cols(c)], buf.at[h, other_rows, cols(c)],
            ag_send.at[unit_id(k, h, c)], ag_recv.at[unit_id(k, h, c)], core_peer,
        ).wait_recv()

    def lin(k, h, c):
        return part[k, h, mine, cols(c)].astype(F32) + xr[k, h, :, cols(c)].astype(F32)

    def hidden_of(h):
        def body(c, _):
            for k in range(2):
                x_copy(k, h, c).wait()
            gate_pre = lin(0, h, c) * scale_gu[1, 0:1, cols(c)]
            up_pre = lin(1, h, c) * scale_gu[1, 1:2, cols(c)]
            hid[h, mine, cols(c)] = (gate_pre * jax.nn.sigmoid(gate_pre) * up_pre).astype(BF16)
            ag_copy(2, hid, h, c).start()
            return 0

        lax.fori_loop(0, nc, body, 0)

    hidden_of(gx)
    hidden_of(1 - gx)

    def hidden_wait(c, _):
        for h in range(2):
            ag_wait(2, hid, h, c)
            ag_copy(2, hid, h, c).wait_send()
        return 0

    lax.fori_loop(0, nc, hidden_wait, 0)

    def low_chunk(c, total):
        return total + contract_last(rows2(hid, slice(None), slice(None), cols(c)), deep[:, cols(c)])

    down_low = lax.fori_loop(0, nc, low_chunk, jnp.zeros((2 * half_t, LANES), F32))
    down_low = jnp.where(is_down, down_low, 0.0)
    back[...] = down_low
    down_low = down_low.astype(BF16)

    sends = (
        (lambda t: (ysend.at[:, tile(t)], yrecv.at[:, tile(t)], y_peer)),
        (lambda t: (ykeep.at[pl.ds(pl.multiple_of((1 - bit0) * quarter, quarter), quarter), tile(t)], z1r.at[:, tile(t)], z1_peer)),
        (lambda t: (z1r.at[pl.ds(pl.multiple_of((1 - bit1) * (quarter // 2), quarter // 2), quarter // 2), tile(t)], z2r.at[:, tile(t)], z2_peer)),
    )
    kept1 = pl.ds(pl.multiple_of(bit0 * quarter, quarter), quarter)
    kept2 = pl.ds(pl.multiple_of(bit1 * (quarter // 2), quarter // 2), quarter // 2)
    peer_block = pl.ds(pl.multiple_of((bit0 * 2 + 1 - bit1) * (quarter // 2), quarter // 2), quarter // 2)
    gone1 = pl.ds(pl.multiple_of((1 - bit0) * quarter, quarter), quarter)

    def yz(v, s, t):
        if s < 3:
            src, dst, peer = sends[s](t)
        elif s == 3:
            src, dst, peer = obuf.at[my_rows, tile(t)], obuf.at[my_rows, tile(t)], z2_peer
        else:
            src, dst, peer = obuf.at[kept1, tile(t)], obuf.at[kept1, tile(t)], z1_peer
        return remote(src, dst, yz_send.at[v, s, t], yz_recv.at[v, s, t], peer)

    def yz_wait(v, s, t):
        if s < 3:
            yz(v, s, t).wait_recv()
        elif s == 3:
            remote(obuf.at[my_rows, tile(t)], obuf.at[peer_block, tile(t)], yz_send.at[v, s, t], yz_recv.at[v, s, t], z2_peer).wait_recv()
        else:
            remote(obuf.at[kept1, tile(t)], obuf.at[gone1, tile(t)], yz_send.at[v, s, t], yz_recv.at[v, s, t], z1_peer).wait_recv()

    def start_tile(v, t, value):
        for h in range(2):
            rows = value[h * half_t : (h + 1) * half_t].astype(BF16)

            @pl.when(h == gx)
            def _():
                ykeep[:, tile(t)] = rows

            @pl.when(h != gx)
            def _():
                ysend[:, tile(t)] = rows

        yz(v, 0, t).start()

    def yz_stage(v, s, t):
        yz_wait(v, s, t)
        if s == 0:
            total = ykeep[:, tile(t)].astype(F32) + yrecv[:, tile(t)].astype(F32)
            ykeep[:, tile(t)] = total.astype(BF16)
        elif s == 1:
            total = ykeep[kept1, tile(t)].astype(F32) + z1r[:, tile(t)].astype(F32)
            z1r[:, tile(t)] = total.astype(BF16)
        elif s == 2:
            total = z1r[kept2, tile(t)].astype(F32) + z2r[:, tile(t)].astype(F32)
            if v == 0:
                dots = cot_mine[:, tile(t)].astype(F32) * total
                gds[place, :, tile(t)] = jnp.sum(dots, axis=0, keepdims=True)
                total = total * scale_dv[:, tile(t)]
            obuf[my_rows, tile(t)] = total.astype(BF16)
        if s < 4:
            yz(v, s + 1, t).start()
        else:
            for n in range(5):
                yz(v, n, t).wait_send()

    def yz_step(v, step, group, spacing):
        for s in range(5):
            t = step - spacing * s

            @pl.when(jnp.logical_and(t >= 0, t < nt // group))
            def _():
                for n in range(group):
                    yz_stage(v, s, t * group + n)

    cot_rows.wait()
    scale_dv = extra.at[0:1, 0:width]
    scale_dv[...] = scale_d

    def down_tile(t, _):
        value = dot(rows2(hid), wd[:, tile(t)]) + dot(down_low, wide[:, tile(t)])
        start_tile(0, t, value)
        return 0

    lax.fori_loop(0, nt, down_tile, 0)

    acc[...] = jnp.zeros_like(acc)
    pl.semaphore_wait(credit.at[0], 1)

    def input_chunk(c, closing=False):
        for h in range(2):
            ag_wait(0, part.at[0], h, c)
            ag_wait(1, part.at[1], h, c)
        gd = rows2(part, 0, slice(None), slice(None), cols(c))
        ud = rows2(part, 1, slice(None), slice(None), cols(c))

        b = deep[:, cols(c)]
        pair = jnp.where(lane2 < rank, contract_last(gd, b), contract_last(ud, b))
        back[...] += jnp.where(lane2 < 2 * rank, pair, 0.0)

        def piece(t):
            return contract_last(gd, wg[tile(t), cols(c)]) + contract_last(ud, wu[tile(t), cols(c)])

        if not closing:

            def body(t, _):
                acc[:, tile(t)] += piece(t)
                return 0

            lax.fori_loop(0, nt, body, 0)
            return
        lb[0] = back[...].astype(BF16)
        back_gu = jnp.where(lane2 < 2 * rank, back[...], 0.0).astype(BF16)
        for n in range(1, 4):
            pl.semaphore_wait(credit.at[n], 1)

        def input_tile(t, _):
            start_tile(1, t, acc[:, tile(t)] + piece(t) + dot(back_gu, wide[:, tile(t)]))
            return 0

        lax.fori_loop(0, nt, input_tile, 0)

    def grads(c, _):
        sums = [None, None]
        for h in range(2):
            x_copy(2, h, c).wait()
            s_g, s_u = scale_gu[1, 0:1, cols(c)], scale_gu[1, 1:2, cols(c)]
            gate_lin, up_lin = lin(0, h, c), lin(1, h, c)
            hgrad = lin(2, h, c).astype(BF16).astype(F32)
            gate_pre, up_pre = gate_lin * s_g, up_lin * s_u
            sig = jax.nn.sigmoid(gate_pre)
            gate_grad = hgrad * up_pre * sig * (1.0 + gate_pre * (1.0 - sig))
            up_grad = hgrad * (gate_pre * sig)
            for k, value in ((0, gate_grad * gate_lin), (1, up_grad * up_lin)):
                piece = jnp.sum(value, axis=0, keepdims=True)
                sums[k] = piece if h == 0 else sums[k] + piece
            part[0, h, mine, cols(c)] = (gate_grad * s_g).astype(BF16)
            part[1, h, mine, cols(c)] = (up_grad * s_u).astype(BF16)
            ag_copy(0, part.at[0], h, c).start()
            ag_copy(1, part.at[1], h, c).start()
        gms[0:1, cols(c)] = sums[0]
        gms[1:2, cols(c)] = sums[1]

        @pl.when(c > 0)
        def _():
            input_chunk(c - 1)

        yz_step(0, c, 2, 1)
        return 0

    lax.fori_loop(0, nc, grads, 0)
    gm_core = remote(gms, gmr, gm_sem.at[0], gm_sem.at[1], core_peer)
    gm_core.start()

    def rest(step, _):
        yz_step(0, step, 2, 1)
        return 0

    lax.fori_loop(nc, max(nc, nt // 2 + 4), rest, 0)
    for n, peer in ((1, y_peer), (2, z1_peer), (3, z2_peer)):
        pl.semaphore_signal(credit.at[n], inc=1, device_id=peer, device_id_type=pl.DeviceIdType.MESH)
    for i in range(1, 8):
        group_copy(gds, i, gd_send, nd_recv.at[1]).start()
    out_copy = pltpu.make_async_copy(obuf, out_hbm, out_sem.at[0])
    out_copy.start()

    input_chunk(nc - 1, closing=True)
    lb_peers = (y_peer, z1_peer, z2_peer)

    def lb_copy(n):
        return remote(lb.at[n], lbr.at[n], lb_send.at[n], lb_recv.at[n], lb_peers[n])

    lb_copy(0).start()
    out_copy.wait()

    la_core.wait_send()
    remote(la.at[1], lar.at[1], la_send.at[1], la_recv.at[1], x_peer).wait()
    la_t = (la[1].astype(F32) + lar[1].astype(F32)).T.astype(BF16)
    ends = []
    cut = hidden_l // 2
    expand_outs = (geg_hbm, geu_hbm, gdr_hbm)
    for k in range(3):
        rows = la_t[k * rank : (k + 1) * rank]
        for j in range(2):
            piece = pl.ds(j * cut, cut)
            if k < 2:
                right = rows2(part, k, slice(None), slice(None), piece)
            else:
                right = rows2(hid, slice(None), slice(None), piece)
            n = k * 2 + j
            if n < 5:
                where = acc.at[(3 + n) * rank : (4 + n) * rank, 0:cut]
            else:
                where = extra.at[:, 0:cut]
            where[...] = dot(rows, right)
            ends.append(pltpu.make_async_copy(where, expand_outs[k].at[:, piece], out_sem.at[8 + n]))
            ends[-1].start()
    low_ends = [
        pltpu.make_async_copy(acc.at[n * rank : (n + 1) * rank], dst, out_sem.at[5 + n])
        for n, dst in enumerate((grg_hbm, gru_hbm, gde_hbm))
    ]

    gm_core.wait()
    gms[...] = (gms[...] + gmr[...]) / scale_gu[0]
    for i in range(hidden_l // LANES):
        for k in range(2):
            gm_out[k, i : i + 1] = gms[k : k + 1, i * LANES : (i + 1) * LANES]
    for i in range(1, 8):
        group_wait(gds, i, gd_send, nd_recv.at[1])
    for i in range(1, 8):
        group_copy(gds, i, gd_send, nd_recv.at[1]).wait_send()
        group_copy(nds, i, nd_send, nd_recv.at[0]).wait_send()
    total, norm = gds[0], nds[0]
    for i in range(1, 8):
        total, norm = total + gds[i], norm + nds[i]
    total = total / jnp.sqrt(jnp.maximum(norm, 0.0) + EPSILON)
    for i in range(width // LANES):
        gd_out[i : i + 1] = total[:, i * LANES : (i + 1) * LANES]
    for i, (src, dst) in enumerate(((gm_out.at[0], gmg_hbm), (gm_out.at[1], gmu_hbm), (gd_out, gdm_hbm))):
        ends.append(pltpu.make_async_copy(src, dst, out_sem.at[2 + i]))
        ends[-1].start()

    def last(step, _):
        @pl.when(step == nt + 7)
        def _():
            lb_t = lb[3].astype(F32).T.astype(BF16)
            acc[0 : 2 * rank] = dot(lb_t[: 2 * rank], rows2(xt))
            acc[2 * rank : 3 * rank] = dot(lb_t[2 * rank : 3 * rank], rows2(dl))
            for copy in low_ends:
                copy.start()

        yz_step(1, step, 1, 2)
        for n in range(3):

            @pl.when(step == nt + 1 + 2 * n)
            def _():
                lb_copy(n).wait()
                lb[n + 1] = (lb[n].astype(F32) + lbr[n].astype(F32)).astype(BF16)
                if n < 2:
                    lb_copy(n + 1).start()

        return 0

    lax.fori_loop(0, nt + 8, last, 0)
    gtok_copy = pltpu.make_async_copy(obuf, gtok_hbm, out_sem.at[1])
    gtok_copy.start()

    for copy in ends + low_ends + [gtok_copy]:
        copy.wait()

    send_cot.wait_send()
    for slot in range(4):
        core_copy(2, slot % 2, nc - 1, slot).wait_send()

    def ag_sends(c, _):
        for h in range(2):
            ag_copy(0, part.at[0], h, c).wait_send()
            ag_copy(1, part.at[1], h, c).wait_send()
        return 0

    lax.fori_loop(0, nc, ag_sends, 0)


def hand_over(*refs):
    sources, targets, stops = refs[:11], refs[11:22], refs[22:33]
    in_sem, out_sem = refs[33:]
    reads = [pltpu.make_async_copy(sources[i], stops[i], in_sem.at[i]) for i in range(11)]
    writes = [pltpu.make_async_copy(stops[i], targets[i], out_sem.at[i]) for i in range(11)]
    for copy in reads:
        copy.start()
    for read, write in zip(reads, writes):
        read.wait()
        write.start()
    for copy in writes:
        copy.wait()


def fits(tokens, gate_weight, gate_expand):
    half_t, width = tokens.shape
    hidden_l, rank = gate_weight.shape[1], gate_expand.shape[0]
    sizes = tuple(lax.axis_size(name) for name in ("gx", "gy", "gz"))
    return (
        sizes == (2, 4, 4)
        and 3 * rank <= LANES
        and rank % 16 == 0
        and half_t % 128 == 0
        and width % LANES == 0
        and 2 * half_t >= 8 * rank
        and width % 512 == 0
        and hidden_l % 512 == 0
        and hidden_l % 256 == 0
        and hidden_l >= 1024
        and hidden_l // 2 <= width
        and 6 * width * hidden_l <= 45 * 2**20
        and half_t * width <= 2**18
    )


def fused(
    tokens, cotangent, gate_weight, up_weight, down_weight, gate_reduce, gate_expand,
    gate_magnitude, up_reduce, up_expand, up_magnitude, down_reduce, down_expand, down_magnitude,
):
    half_t, width = tokens.shape
    hidden_l, rank = gate_weight.shape[1], gate_expand.shape[0]
    all_t, quarter = 2 * half_t, half_t // 2
    fc, dt = 512, 256
    nc, nt = hidden_l // fc, width // dt
    any_space = pl.BlockSpec(memory_space=pl.ANY)
    dma = pltpu.SemaphoreType.DMA
    units = 6 * nc
    rows_f, rows_d = hidden_l // LANES, width // LANES
    shapes = (
        ((half_t, width), BF16), ((half_t, width), BF16),
        ((rank, width), F32), ((rank, width), F32), ((rank, width), F32),
        ((rank, hidden_l), F32), ((rank, hidden_l), F32), ((rank, hidden_l), F32),
        ((rows_f, LANES), F32), ((rows_f, LANES), F32), ((rows_d, LANES), F32),
    )
    results = pl.pallas_call(
        kernel,
        out_shape=[jax.ShapeDtypeStruct(*pair) for pair in shapes],
        in_specs=[any_space] * 14,
        out_specs=[any_space] * 11,
        scratch_shapes=[
            pltpu.VMEM((LANES, width), BF16),
            pltpu.VMEM((LANES, hidden_l), BF16),
            pltpu.VMEM((2, rows_f, LANES), F32),
            pltpu.VMEM((rows_d, LANES), F32),
            pltpu.VMEM((2, rows_f, LANES), F32),
            pltpu.VMEM((rows_d, LANES), F32),
            pltpu.VMEM((width, hidden_l), BF16),
            pltpu.VMEM((width, hidden_l), BF16),
            pltpu.VMEM((hidden_l, width), BF16),
            pltpu.VMEM((2, half_t, width), BF16),
            pltpu.VMEM((2, half_t, width), BF16),
            pltpu.VMEM((3, 2, half_t, hidden_l), BF16),
            pltpu.VMEM((3, 2, quarter, hidden_l), BF16),
            pltpu.VMEM((2, half_t, hidden_l), BF16),
            pltpu.VMEM((4, quarter, fc), BF16),
            pltpu.VMEM((all_t, width), F32),
            pltpu.VMEM((half_t, width), BF16),
            pltpu.VMEM((half_t, width), BF16),
            pltpu.VMEM((half_t, width), BF16),
            pltpu.VMEM((quarter, width), BF16),
            pltpu.VMEM((quarter // 2, width), BF16),
            pltpu.VMEM((half_t, width), BF16),
            pltpu.VMEM((half_t // 4, width), BF16),
            pltpu.VMEM((2, half_t, LANES), F32),
            pltpu.VMEM((2, all_t, LANES), BF16),
            pltpu.VMEM((2, all_t, LANES), BF16),
            pltpu.VMEM((all_t, LANES), F32),
            pltpu.VMEM((4, all_t, LANES), BF16),
            pltpu.VMEM((3, all_t, LANES), BF16),
            pltpu.VMEM((8, 1, width), F32),
            pltpu.VMEM((4, 2, hidden_l), F32),
            pltpu.VMEM((2, 2, hidden_l), F32),
            pltpu.VMEM((2, hidden_l), F32),
            pltpu.VMEM((2, hidden_l), F32),
            pltpu.VMEM((8, 1, width), F32),
            pltpu.VMEM((rank, width), F32),
            dma((3, nc)),
            dma((12,)),
            dma((2,)),
            dma((2,)),
            dma((4,)),
            dma((units,)),
            dma((units,)),
            dma((units,)),
            dma((units,)),
            dma((units,)),
            dma((2, 5, nt)),
            dma((2, 5, nt)),
            dma((7,)),
            dma((7,)),
            dma((2, 8)),
            dma((3,)),
            dma((4,)),
            dma((2,)),
            dma((2,)),
            dma((3,)),
            dma((3,)),
            dma((2,)),
            dma((14,)),
            pltpu.SemaphoreType.REGULAR((4,)),
        ],
        compiler_params=pltpu.CompilerParams(
            collective_id=0, has_side_effects=True, vmem_limit_bytes=67043328
        ),
    )(
        tokens, cotangent, gate_weight, up_weight, down_weight, gate_reduce.T, up_reduce.T,
        down_expand, gate_expand, up_expand, down_reduce.T, gate_magnitude.reshape(rows_f, LANES),
        up_magnitude.reshape(rows_f, LANES), down_magnitude.reshape(rows_d, LANES),
    )
    results = pl.pallas_call(
        hand_over,
        out_shape=[jax.ShapeDtypeStruct(*pair) for pair in shapes],
        in_specs=[pl.BlockSpec(memory_space=pltpu.HBM)] * 11,
        out_specs=[pl.BlockSpec(memory_space=pltpu.HBM)] * 11,
        scratch_shapes=[pltpu.VMEM(*pair) for pair in shapes] + [dma((11,)), dma((11,))],
        compiler_params=pltpu.CompilerParams(vmem_limit_bytes=67043328),
    )(*results)
    output, grad_tokens, grg, gru, gde, geg, geu, gdr, gmg, gmu, gdm = results
    return (
        output, grad_tokens, grg.T, geg, gmg.reshape(-1), gru.T, geu, gmu.reshape(-1),
        gdr.T, gde, gdm.reshape(-1),
    )


def choose_body(mesh):
    def body(*args):
        if fits(args[0], args[2], args[6]):
            return fused(*args)
        return on_device(*args)

    return body


def solution(mesh):
    return jax.shard_map(
        choose_body(mesh),
        mesh=mesh,
        in_specs=(
            P("gx", "gy"),
            P("gx", "gy"),
            P("gy", ("gx", "gz")),
            P("gy", ("gx", "gz")),
            P(("gx", "gz"), "gy"),
            P("gy", None),
            P(None, ("gx", "gz")),
            P(("gx", "gz")),
            P("gy", None),
            P(None, ("gx", "gz")),
            P(("gx", "gz")),
            P(("gx", "gz"), None),
            P(None, "gy"),
            P("gy"),
        ),
        out_specs=(
            P("gx", "gy"),
            P("gx", "gy"),
            P("gy", None),
            P(None, ("gx", "gz")),
            P(("gx", "gz")),
            P("gy", None),
            P(None, ("gx", "gz")),
            P(("gx", "gz")),
            P(("gx", "gz"), None),
            P(None, "gy"),
            P("gy"),
        ),
        check_vma=False,
    )
```
